32 devices in a mesh: dp: 16 (over z, y, core), tensor: 2 (over x).
Axes of the slice: x: 2, y: 2, z: 4, core: 2. Of those that a mesh axis runs over, the one named last changes fastest.
Arguments:
- content: bfloat16 [16384, 768], P('dp'), may hold values from -6 to 6
- query_stream: bfloat16 [2560, 768], P('dp'), may hold values from -6 to 6
- factor_order: int32 [32, 512], P('dp'), may hold values from 0 to 511, each once within a row
- query_weight: bfloat16 [768, 768], P(None, 'tensor'), may hold values from -0.21875 to 0.21875
- key_weight: bfloat16 [768, 768], P(None, 'tensor'), may hold values from -0.21875 to 0.21875
- value_weight: bfloat16 [768, 768], P(None, 'tensor'), may hold values from -0.21875 to 0.21875
- output_weight: bfloat16 [768, 768], P('tensor'), may hold values from -1.75 to 1.75
- up_weight: bfloat16 [768, 3072], P(None, 'tensor'), may hold values from -0.21875 to 0.21875
- down_weight: bfloat16 [3072, 768], P('tensor'), may hold values from -0.109375 to 0.109375
- query_bias: float32 [768], P('tensor'), may hold values from -1.75 to 1.75
- value_bias: float32 [768], P('tensor'), may hold values from -1.75 to 1.75
- up_bias: float32 [3072], P('tensor'), may hold values from -1.75 to 1.75
- output_bias: float32 [768], replicated, may hold values from -1.75 to 1.75
- down_bias: float32 [768], replicated, may hold values from -1.75 to 1.75
- first_gain: float32 [768], replicated, may hold values from 0.25 to 1.75
- first_shift: float32 [768], replicated, may hold values from -1.75 to 1.75
- second_gain: float32 [768], replicated, may hold values from 0.25 to 1.75
- second_shift: float32 [768], replicated, may hold values from -1.75 to 1.75
- bucket_table: float32 [32, 12], P(None, 'tensor'), may hold values from -6 to 6
- content_cotangent: bfloat16 [16384, 768], P('dp'), may hold values from -6 to 6
- query_cotangent: bfloat16 [2560, 768], P('dp'), may hold values from -6 to 6
Outputs:
- content_output: bfloat16 [16384, 768], P('dp')
- query_output: bfloat16 [2560, 768], P('dp')
- content_gradient: float32 [16384, 768], P('dp')
- query_gradient: float32 [2560, 768], P('dp')
- query_weight_gradient: float32 [768, 768], P('dp', 'tensor')
- key_weight_gradient: float32 [768, 768], P('dp', 'tensor')
- value_weight_gradient: float32 [768, 768], P('dp', 'tensor')
- output_weight_gradient: float32 [768, 768], P('tensor', 'dp')
- up_weight_gradient: float32 [768, 3072], P('dp', 'tensor')
- down_weight_gradient: float32 [3072, 768], P('tensor', 'dp')
- query_bias_gradient: float32 [768], P('tensor')
- value_bias_gradient: float32 [768], P('tensor')
- up_bias_gradient: float32 [3072], P('tensor')
- table_gradient: float32 [32, 12], P(None, 'tensor')
- output_bias_gradient: float32 [768], P('dp')
- down_bias_gradient: float32 [768], P('dp')
- first_gain_gradient: float32 [768], P('dp')
- first_shift_gradient: float32 [768], P('dp')
- second_gain_gradient: float32 [768], P('dp')
- second_shift_gradient: float32 [768], P('dp')
The draws below stay inside these ranges and needn't reach their ends.
Inputs may be any that keep to these rules, and one draw needn't show every extreme that they name: Each row of factor_order holds every position 0 to 511 once; factor_order[s, k] is the position that comes k-th in sequence s.
All inputs are finite; a program needn't handle non-finite values.
Results may differ from the reference program's by a relative error of at most 0.015.
The reference program's roundings to bfloat16 on the way count: a program that leaves them out, or rounds other values in their place, can miss the bound.
Values may be sent and summed in bfloat16 or wider, within the bound.
A program may use at most 192 MiB of HBM per device.

```python
import jax
import jax.numpy as jnp
from jax import lax

D = 768
H = 12
HD = 64
FF = 3072
NB = 32
S = 512
SEQS = 32
TOKENS = 16384
QROWS = 2560


def spiked(array, own_key, source, target, blocks, factor):
    def block_of(position):
        return (jnp.arange(array.shape[position]) // (array.shape[position] // blocks)).reshape((-1,) + (1,) * (array.ndim - 1 - position))

    one_side = jax.random.permutation(own_key, blocks)[block_of(target)]
    other_side = (block_of(target) + blocks // 2) % blocks
    return jnp.where((block_of(source) == one_side) | (block_of(source) == other_side), factor * array, array)


def block_scale(rng, shape, split, smallest, top_value):
    def one(axis_at, shards_of):
        steps = jax.random.uniform(jax.random.fold_in(jax.random.fold_in(rng, 6), axis_at), (shards_of,), jnp.float32, smallest / len(split), top_value / len(split))
        return jnp.repeat(jnp.exp(steps), shape[axis_at] // shards_of).reshape((-1,) + (1,) * (len(shape) - axis_at - 1))

    factor_of = one(*split[0])
    for cut in split[1:]:
        factor_of = factor_of * one(*cut)
    return factor_of


def noise(own_key, dims, deviation, bound, pieces=(), held_as=jnp.bfloat16):
    factor_of = block_scale(own_key, dims, pieces, -0.22, 0.18) if pieces else 1.0
    entries = jax.random.normal(own_key, dims, jnp.float32) * deviation * factor_of
    return jnp.minimum(jnp.maximum(entries, -bound), bound).astype(held_as)


def heavy_noise(rng, dims, deviation, most, cuts, heavy, kind=jnp.bfloat16):
    entries = deviation * jax.random.normal(rng, dims, jnp.float32)
    if cuts:
        entries = entries * block_scale(rng, dims, cuts, -0.22, 0.18)
    return jnp.clip(spiked(entries, jax.random.fold_in(rng, 3), *heavy), -most, most).astype(kind)


def setup_inputs(seed: int = 0) -> dict:
    streams_of = jax.random.split(jax.random.key(seed), 22)
    return {
        "content": heavy_noise(streams_of[0], (TOKENS, D), 1.0, 6.0, ((0, 16),), (0, 1, 16, 2.0)),
        "query_stream": heavy_noise(streams_of[1], (QROWS, D), 1.0, 6.0, ((0, 16),), (0, 1, 16, 2.0)),
        "factor_order": jax.vmap(lambda own: jax.random.permutation(own, S))(jax.random.split(streams_of[2], SEQS)).reshape((SEQS, S)).astype(jnp.int32),
        "query_weight": noise(streams_of[3], (D, H * HD), D ** -0.5, 0.21875, ((1, 2),)),
        "key_weight": noise(streams_of[4], (D, H * HD), D ** -0.5, 0.21875, ((1, 2),)),
        "value_weight": noise(streams_of[5], (D, H * HD), D ** -0.5, 0.21875, ((1, 2),)),
        "output_weight": noise(streams_of[6], (H * HD, D), (max(4, H * HD // 64)) ** -0.5, 1.75, ((0, 2),)),
        "up_weight": noise(streams_of[7], (D, FF), D ** -0.5, 0.21875, ((1, 2),)),
        "down_weight": noise(streams_of[8], (FF, D), FF ** -0.5, 0.109375, ((0, 2),)),
        "query_bias": noise(streams_of[9], (H * HD,), 0.3, 1.75, ((0, 2),), jnp.float32),
        "value_bias": noise(streams_of[10], (H * HD,), 0.3, 1.75, ((0, 2),), jnp.float32),
        "up_bias": noise(streams_of[11], (FF,), 0.3, 1.75, ((0, 2),), jnp.float32),
        "output_bias": noise(streams_of[12], (D,), 0.3, 1.75, (), jnp.float32),
        "down_bias": noise(streams_of[13], (D,), 0.3, 1.75, (), jnp.float32),
        "first_gain": jnp.clip(1.0 + 0.15 * jax.random.normal(streams_of[14], (D,), jnp.float32), 0.25, 1.75),
        "first_shift": noise(streams_of[15], (D,), 0.3, 1.75, (), jnp.float32),
        "second_gain": jnp.clip(1.0 + 0.15 * jax.random.normal(streams_of[16], (D,), jnp.float32), 0.25, 1.75),
        "second_shift": noise(streams_of[17], (D,), 0.3, 1.75, (), jnp.float32),
        "bucket_table": noise(streams_of[18], (NB, H), 1.0, 6.0, ((1, 2),), jnp.float32),
        "content_cotangent": heavy_noise(streams_of[19], (TOKENS, D), 1.0, 6.0, ((0, 16),), (0, 1, 16, 2.0)),
        "query_cotangent": heavy_noise(streams_of[20], (QROWS, D), 1.0, 6.0, ((0, 16),), (0, 1, 16, 2.0)),
    }


@jax.custom_vjp
def low(v):
    return lax.optimization_barrier(v.astype(jnp.bfloat16)).astype(jnp.float32)

@jax.custom_vjp
def low_back(v):
    return v

def low_keep(v):
    return (low(v), None)

def low_pass(kept, grad):
    return (grad,)

def back_keep(v):
    return (v, None)

def back_low(kept, grad):
    return (low(grad),)
low.defvjp(low_keep, low_pass)
low_back.defvjp(back_keep, back_low)
PRECISE = lax.Precision.HIGHEST
NEG_BIG = -1e+30
EPSILON = 1e-05
THRESHOLDS = (12, 16, 23, 32, 46, 64, 91)

def both_round(operand):
    return low(low_back(operand))

def bucket_index(length):
    positions = jnp.arange(length, dtype=jnp.int32)
    offset = positions[None, :] - positions[:, None]
    distance = jnp.abs(offset)
    result = jnp.minimum(distance, 8)
    for threshold in THRESHOLDS:
        result = result + (distance >= threshold).astype(jnp.int32)
    return result + 16 * (offset > 0).astype(jnp.int32)

def visibility(factor_row, length, predict):
    positions = jnp.arange(length, dtype=jnp.int32)
    matches = factor_row[:, None] == positions[None, :]
    order_rank = lax.optimization_barrier(jnp.sum(jnp.where(matches, positions[:, None], 0), axis=0)).astype(jnp.int32)
    picked = factor_row[length - predict:]
    content_limit = jnp.maximum(order_rank, length - predict - 1)
    see_content = order_rank[None, :] <= content_limit[:, None]
    stream_limit = length - predict + jnp.arange(predict, dtype=jnp.int32)
    see_stream = order_rank[None, :] < stream_limit[:, None]
    return (see_content, see_stream, picked)

def masked_softmax(scores, visible):
    scores = jnp.where(visible[None], scores, NEG_BIG)
    row_max = lax.optimization_barrier(jnp.max(scores, axis=-1, keepdims=True))
    exponent = jnp.exp(scores - row_max)
    return exponent / lax.optimization_barrier(jnp.sum(exponent, axis=-1, keepdims=True))

def normalize(residual, gain_vector, shift_vector):
    center = residual - lax.optimization_barrier(jnp.mean(residual, axis=-1, keepdims=True))
    spread = lax.optimization_barrier(jnp.mean(center * center, axis=-1, keepdims=True))
    return center * lax.rsqrt(spread + EPSILON) * gain_vector + shift_vector

def forward(content, query_stream, query_weight, key_weight, value_weight, output_weight, up_weight, down_weight, query_bias, value_bias, up_bias, output_bias, down_bias, first_gain, first_shift, second_gain, second_shift, bucket_table, factor_order):
    sequences, length = factor_order.shape
    predict = query_stream.shape[0] // sequences
    head_count = bucket_table.shape[1]
    head_size = query_weight.shape[1] // head_count
    inner_width = head_count * head_size
    content_query = both_round(jnp.dot(content, query_weight, precision=PRECISE) + query_bias)
    content_key = both_round(jnp.dot(content, key_weight, precision=PRECISE))
    content_value = both_round(jnp.dot(content, value_weight, precision=PRECISE) + value_bias)
    stream_query = both_round(jnp.dot(query_stream, query_weight, precision=PRECISE) + query_bias)
    position_bias = jnp.transpose(jnp.take(bucket_table, bucket_index(length), axis=0), (2, 0, 1))

    def attend(blocks):
        query_block, stream_block, key_block, value_block, factor_row = blocks
        see_content, see_stream, picked = visibility(factor_row, length, predict)
        scores = jnp.einsum('qhd,khd->hqk', query_block, key_block, precision=PRECISE) * 0.125 + position_bias
        weights = low(masked_softmax(low_back(scores), see_content))
        mixed_rows = jnp.einsum('hqk,khd->qhd', weights, value_block, precision=PRECISE)
        stream_scores = jnp.einsum('qhd,khd->hqk', stream_block, key_block, precision=PRECISE) * 0.125 + jnp.take(position_bias, picked, axis=1)
        stream_weights = low(masked_softmax(low_back(stream_scores), see_stream))
        stream_mixed = jnp.einsum('hqk,khd->qhd', stream_weights, value_block, precision=PRECISE)
        return (mixed_rows.reshape(length, inner_width), stream_mixed.reshape(predict, inner_width))
    blocks = (content_query.reshape(sequences, length, head_count, head_size), stream_query.reshape(sequences, predict, head_count, head_size), content_key.reshape(sequences, length, head_count, head_size), content_value.reshape(sequences, length, head_count, head_size), factor_order)
    mixed_content, mixed_stream = lax.map(jax.checkpoint(attend), blocks)
    mixed_all = both_round(jnp.concatenate([mixed_content.reshape(-1, inner_width), mixed_stream.reshape(-1, inner_width)], axis=0))
    inputs_all = jnp.concatenate([content, query_stream], axis=0)
    branch = low_back(jnp.dot(mixed_all, output_weight, precision=PRECISE))
    first_out = normalize(inputs_all + branch + output_bias, first_gain, first_shift)
    hidden_pre = low_back(jnp.dot(low(first_out), up_weight, precision=PRECISE) + up_bias)
    hidden = low(jax.nn.gelu(hidden_pre, approximate=False))
    feed_out = low_back(jnp.dot(hidden, down_weight, precision=PRECISE))
    final_out = normalize(first_out + feed_out + down_bias, second_gain, second_shift)
    token_rows = content.shape[0]
    return (final_out[:token_rows], final_out[token_rows:])

def reference(content, query_stream, factor_order, query_weight, key_weight, value_weight, output_weight, up_weight, down_weight, query_bias, value_bias, up_bias, output_bias, down_bias, first_gain, first_shift, second_gain, second_shift, bucket_table, content_cotangent, query_cotangent):
    floats = tuple((operand.astype(jnp.float32) for operand in (content, query_stream, query_weight, key_weight, value_weight, output_weight, up_weight, down_weight, query_bias, value_bias, up_bias, output_bias, down_bias, first_gain, first_shift, second_gain, second_shift, bucket_table)))

    def wrapped(*params):
        return forward(*params, factor_order)
    outputs, pullback = jax.vjp(wrapped, *floats)
    gradients = pullback((content_cotangent.astype(jnp.float32), query_cotangent.astype(jnp.float32)))
    return (outputs[0].astype(jnp.bfloat16), outputs[1].astype(jnp.bfloat16), gradients[0], gradients[1], gradients[2], gradients[3], gradients[4], gradients[5], gradients[6], gradients[7], gradients[8], gradients[9], gradients[10], gradients[17], gradients[11], gradients[12], gradients[13], gradients[14], gradients[15], gradients[16])
```

```python
import jax
import jax.numpy as jnp
from jax import lax
from jax.experimental import pallas as pl
from jax.experimental.pallas import tpu as pltpu
from jax.sharding import PartitionSpec as P

F32 = jnp.float32
BF = jnp.bfloat16
PRECISE = lax.Precision.HIGHEST
EPSILON = 1e-05
THRESHOLDS = (12, 16, 23, 32, 46, 64, 91)


def mm(a,b,ca,cb):
    return lax.dot_general(a,b,(((ca,),(cb,)),((),())),preferred_element_type=F32)

def attend_kernel(picked, x_ref, wq_ref, wk_ref, wv_ref, qb_ref, vb_ref, rank_ref, limit_ref, off_ref,
                  q_ref, k_ref, v_ref, w_ref, m_ref, bias_ref):
    rows=x_ref.shape[0]; length=rank_ref.shape[1]; predict=rows-length; hd=q_ref.shape[1]//2
    x=x_ref[...]
    q=(mm(x,wq_ref[...],1,0)+qb_ref[...]).astype(BF)
    k=mm(x[:length],wk_ref[...],1,0).astype(BF)
    v=(mm(x[:length],wv_ref[...],1,0)+vb_ref[...]).astype(BF)
    q_ref[...]=q; k_ref[...]=k; v_ref[...]=v
    first=lax.broadcasted_iota(jnp.int32,(1,2*hd),1)<hd
    visible=rank_ref[...]<=limit_ref[...]
    parts=[]
    for a in range(2):
        wide=jnp.broadcast_to(off_ref[0,a:a+1,:],(length,2*length))
        turned=pltpu.roll(wide,0,1,stride=1,stride_axis=0)
        bias_ref[:length,:]=turned[:,length:]
        def row(p,c):
            bias_ref[pl.ds(length+p,1),:]=bias_ref[pl.ds(picked[p],1),:]
            return c
        lax.fori_loop(0,predict,row,0,unroll=8)
        mask=first if a==0 else jnp.logical_not(first)
        qa=jnp.where(mask,q,jnp.zeros_like(q))
        s=mm(qa,k,1,1)*0.125+bias_ref[...]
        s=jnp.where(visible,s,-1e30)
        e=jnp.exp(s-jnp.max(s,axis=1,keepdims=True))
        w=(e/jnp.sum(e,axis=1,keepdims=True)).astype(BF)
        w_ref[a]=w
        parts.append(mm(w,v,1,0))
    m_ref[...]=jnp.where(first,parts[0],parts[1]).astype(BF)

def attend(x,wq,wk,wv,qb,vb,rank,limit,off,picked):
    rows,d=x.shape; length=rank.shape[1]; inner=wq.shape[1]; pairs=off.shape[0]; pw=inner//pairs
    col=lambda n:pl.BlockSpec((n,pw),lambda h,p:(0,h))
    full=lambda a:pl.BlockSpec(a.shape,lambda h,p:(0,)*a.ndim)
    s=jax.ShapeDtypeStruct
    return pl.pallas_call(attend_kernel,
        out_shape=(s((rows,inner),BF),s((length,inner),BF),s((length,inner),BF),s((2*pairs,rows,length),BF),s((rows,inner),BF)),
        grid_spec=pltpu.PrefetchScalarGridSpec(num_scalar_prefetch=1,grid=(pairs,),
            in_specs=[full(x),col(d),col(d),col(d),col(1),col(1),full(rank),full(limit),pl.BlockSpec((1,)+off.shape[1:],lambda h,p:(h,0,0))],
            out_specs=(col(rows),col(length),col(length),pl.BlockSpec((2,rows,length),lambda h,p:(h,0,0)),col(rows)),
            scratch_shapes=[pltpu.VMEM((rows,length),F32)]),
        compiler_params=pltpu.CompilerParams(vmem_limit_bytes=56<<20),
        cost_estimate=pl.CostEstimate(flops=2*rows*d*inner*3+4*rows*length*inner,bytes_accessed=20<<20,transcendentals=rows*length*2*pairs),
        name="attend")(picked,x,wq,wk,wv,qb,vb,rank,limit,off)

def back_kernel(g_ref, wo_ref, q_ref, k_ref, v_ref, w_ref, flip_ref, dq_ref, dk_ref, dv_ref, t_ref):
    rows=g_ref.shape[0]; length=k_ref.shape[0]; predict=rows-length; hd=q_ref.shape[1]//2
    do=mm(g_ref[...],wo_ref[...],1,1).astype(BF)
    q=q_ref[...]; k=k_ref[...]; v=v_ref[...]
    first=lax.broadcasted_iota(jnp.int32,(1,2*hd),1)<hd
    dq=[];dk=[];dv=[]
    for a in range(2):
        mask=first if a==0 else jnp.logical_not(first)
        doa=jnp.where(mask,do,jnp.zeros_like(do))
        wl=w_ref[a]; w=wl.astype(F32)
        dw=mm(doa,v,1,1)
        centre=jnp.sum(dw*w,axis=1,keepdims=True)
        ds=(w*(dw-centre)).astype(BF)
        dq.append(mm(ds,k,1,0)); dk.append(mm(ds,q,0,0)); dv.append(mm(wl,do,0,0))
        flipped=mm(flip_ref[...],ds,1,0)
        wide=jnp.concatenate([flipped,jnp.zeros((length,length),F32)],axis=1)
        turned=pltpu.roll(wide,0,1,stride=1,stride_axis=0)
        t_ref[0,a:a+1,:]=jnp.sum(turned,axis=0,keepdims=True)
    dq_ref[...]=(jnp.where(first,dq[0],dq[1])*0.125).astype(BF)
    dk_ref[...]=(jnp.where(first,dk[0],dk[1])*0.125).astype(BF)
    dv_ref[...]=jnp.where(first,dv[0],dv[1]).astype(BF)

def attend_back(g,wo,q,k,v,w,flip):
    rows,d=g.shape; length,inner=k.shape; pairs=w.shape[0]//2; pw=inner//pairs
    col=lambda n:pl.BlockSpec((n,pw),lambda h:(0,h))
    s=jax.ShapeDtypeStruct
    return pl.pallas_call(back_kernel,
        out_shape=(s((rows,inner),BF),s((length,inner),BF),s((length,inner),BF),s((pairs,2,2*length),F32)),
        grid=(pairs,),
        in_specs=[pl.BlockSpec((rows,d),lambda h:(0,0)),pl.BlockSpec((pw,d),lambda h:(h,0)),col(rows),col(length),col(length),pl.BlockSpec((2,rows,length),lambda h:(h,0,0)),pl.BlockSpec(flip.shape,lambda h:(0,0))],
        out_specs=(col(rows),col(length),col(length),pl.BlockSpec((1,2,2*length),lambda h:(h,0,0))),
        compiler_params=pltpu.CompilerParams(vmem_limit_bytes=56<<20),
        cost_estimate=pl.CostEstimate(flops=2*rows*d*inner+10*rows*length*inner,bytes_accessed=20<<20,transcendentals=0),
        name="attend_back")(g,wo,q,k,v,w,flip)


def norm_forward(residual, gain_vector, shift_vector):
    center = residual - jnp.mean(residual, axis=-1, keepdims=True)
    spread = jnp.mean(center * center, axis=-1, keepdims=True)
    inverse = lax.rsqrt(spread + EPSILON)
    normed = center * inverse
    return (normed * gain_vector + shift_vector, normed, inverse)


def norm_backward(upstream, normed, inverse, gain_vector):
    scaled = upstream * gain_vector
    inner_term = (
        scaled
        - jnp.mean(scaled, axis=-1, keepdims=True)
        - normed * jnp.mean(scaled * normed, axis=-1, keepdims=True)
    )
    return (inner_term * inverse, jnp.sum(upstream * normed, axis=0), jnp.sum(upstream, axis=0))


def gelu_exact(operand):
    return jax.nn.gelu(operand, approximate=False)


def offset_onehot(slots, length):
    offset = jnp.arange(2 * length, dtype=jnp.int32) - length
    distance = jnp.abs(offset)
    bucket = jnp.minimum(distance, 8)
    for threshold in THRESHOLDS:
        bucket = bucket + (distance >= threshold).astype(jnp.int32)
    bucket = bucket + 16 * (offset > 0).astype(jnp.int32)
    return (bucket[None, :] == jnp.arange(slots, dtype=jnp.int32)[:, None]).astype(F32)


def pick(matrix, index, count):
    return lax.dynamic_slice_in_dim(matrix, index * count, count, 0)


def across(value):
    return lax.ppermute(value, "tensor", [(0, 1), (1, 0)])


def swap(value, bit):
    return lax.ppermute(value, "dp", [(i, i ^ bit) for i in range(lax.axis_size("dp"))])


def other_half(shard, core):
    halves = shard.reshape((2, shard.shape[0] // 2) + shard.shape[1:])
    got = across(lax.dynamic_index_in_dim(halves, core, 0, keepdims=False))
    traded = swap(got, 1)
    low = jnp.where(core == 0, got, traded)
    high = jnp.where(core == 0, traded, got)
    return jnp.concatenate([low, high], axis=0)


def halve(blocks, bit_index, group):
    n, rows, columns = blocks.shape
    split = blocks.reshape(n // 2, 2, rows, columns)
    mine = (group >> bit_index) & 1
    keep = lax.dynamic_index_in_dim(split, mine, 1, keepdims=False)
    give = lax.dynamic_index_in_dim(split, 1 - mine, 1, keepdims=False)
    got = swap(give, 1 << bit_index)
    return (keep.astype(F32) + got.astype(F32)).astype(BF)


def join(own, oth):
    return (own.astype(F32) + across(oth).astype(F32)).astype(BF)


def body(
    content,
    query_stream,
    factor_order,
    query_weight,
    key_weight,
    value_weight,
    output_weight,
    up_weight,
    down_weight,
    query_bias,
    value_bias,
    up_bias,
    output_bias,
    down_bias,
    first_gain,
    first_shift,
    second_gain,
    second_shift,
    bucket_table,
    content_cotangent,
    query_cotangent,
):
    side = lax.axis_index("tensor")
    group = lax.axis_index("dp")
    group_count = lax.axis_size("dp")
    bits = group_count.bit_length() - 1
    core = group & 1
    length = factor_order.shape[1]
    predict = query_stream.shape[0] // factor_order.shape[0]
    seqs = factor_order.shape[0] // 2
    x = jnp.concatenate(
        [pick(content, side, seqs * length), pick(query_stream, side, seqs * predict)], axis=0
    )
    upstream = jnp.concatenate(
        [pick(content_cotangent, side, seqs * length), pick(query_cotangent, side, seqs * predict)],
        axis=0,
    )
    order = pick(factor_order, side, seqs)[0]
    width = x.shape[1]
    inner = query_weight.shape[1]
    heads = bucket_table.shape[1]
    slots = bucket_table.shape[0]

    packed = jnp.concatenate([query_bias, value_bias, up_bias, bucket_table.T.reshape(-1)])
    far = across(packed)

    def unpack(vector):
        a, b, c = inner, 2 * inner, 2 * inner + up_bias.shape[0]
        return vector[:a], vector[a:b], vector[b:c], vector[c:].reshape(heads, slots)

    qkv = jnp.stack([query_weight, key_weight, value_weight])
    qkv_far = other_half(qkv.reshape(3 * width, inner), core).reshape(3, width, inner)
    out_far = other_half(output_weight, core)
    up_far = other_half(up_weight, core)
    down_far = other_half(down_weight, core)

    onehot = offset_onehot(slots, length)
    positions = jnp.arange(length, dtype=jnp.int32)
    rank = jnp.sum(
        jnp.where(order[:, None] == positions[None, :], positions[:, None], 0), axis=0
    ).astype(jnp.int32)
    picked = order[length - predict :]
    limit = jnp.concatenate(
        [
            jnp.maximum(rank, length - predict - 1),
            length - predict - 1 + jnp.arange(predict, dtype=jnp.int32),
        ]
    )[:, None]
    rank = rank[None, :]
    source = jnp.concatenate([positions, picked])
    flip = (source[None, :] == length - 1 - positions[:, None]).astype(BF)

    def attend_half(weights, small):
        qb, vb, _, table = small
        offsets = jnp.einsum("hb,bn->hn", table, onehot, precision=PRECISE)
        return attend(
            x,
            weights[0],
            weights[1],
            weights[2],
            qb[None, :],
            vb[None, :],
            rank,
            limit,
            offsets.reshape(heads // 2, 2, 2 * length),
            picked,
        )

    near_small = unpack(packed)
    far_small = unpack(far)
    q0, k0, v0, w0, m0 = attend_half((query_weight, key_weight, value_weight), near_small)
    q1, k1, v1, w1, m1 = attend_half((qkv_far[0], qkv_far[1], qkv_far[2]), far_small)

    def dot(a, b):
        return jnp.dot(a, b, preferred_element_type=F32)

    def dot_t(a, b):
        return lax.dot_general(a, b, (((1,), (1,)), ((), ())), preferred_element_type=F32)

    def grad(a, b):
        return lax.dot_general(a, b, (((0,), (0,)), ((), ())), preferred_element_type=F32)

    branch = dot(m0, output_weight) + dot(m1, out_far)
    first_out, first_normed, first_inverse = norm_forward(
        x.astype(F32) + branch + output_bias, first_gain, first_shift
    )
    first_low = first_out.astype(BF)

    def hidden_of(weight, bias):
        pre = dot(first_low, weight) + bias
        value, pull = jax.vjp(gelu_exact, pre)
        return value.astype(BF), pull

    h0, pull0 = hidden_of(up_weight, near_small[2])
    h1, pull1 = hidden_of(up_far, far_small[2])
    feed = dot(h0, down_weight) + dot(h1, down_far)
    final_out, second_normed, second_inverse = norm_forward(
        first_out + feed + down_bias, second_gain, second_shift
    )
    final_low = final_out.astype(BF)
    final_far = across(final_low)
    second_grad, second_gain_grad, second_shift_grad = norm_backward(
        upstream.astype(F32), second_normed, second_inverse, second_gain
    )
    second_low = second_grad.astype(BF)
    down_bias_grad = jnp.sum(second_grad, axis=0)

    def blocks(matrix):
        rows, columns = matrix.shape
        return matrix.astype(BF).reshape(group_count, rows // group_count, columns)

    down0 = blocks(grad(second_low, h0))
    down1 = blocks(grad(second_low, h1))
    down_g = jnp.concatenate([down0, down1], axis=2)
    for bit in range(bits):
        down_g = halve(down_g, bit, group)
    down_g = down_g[0]
    units = down_weight.shape[0]
    down_final = down_g[:, :units].astype(F32) + across(down_g[:, units:]).astype(F32)

    (pre0,) = pull0(dot_t(second_low, down_weight))
    (pre1,) = pull1(dot_t(second_low, down_far))
    p0 = pre0.astype(BF)
    p1 = pre1.astype(BF)
    up0 = blocks(grad(first_low, p0))
    up1 = blocks(grad(first_low, p1))
    up_g = join(halve(up0, 0, group), halve(up1, 0, group))
    for bit in range(1, bits):
        up_g = halve(up_g, bit, group)
    up_bias0 = jnp.sum(p0.astype(F32), axis=0)
    up_bias1 = jnp.sum(p1.astype(F32), axis=0)
    back = dot_t(p0, up_weight) + dot_t(p1, up_far)
    first_grad, first_gain_grad, first_shift_grad = norm_backward(
        second_grad + back, first_normed, first_inverse, first_gain
    )
    first_low_grad = first_grad.astype(BF)
    output_bias_grad = jnp.sum(first_grad, axis=0)

    def sum_all(same, own, oth):
        cut = same.shape[0]
        got = across(jnp.concatenate([same, oth]))
        total = jnp.concatenate([same, own]) + got
        for bit in range(bits):
            total = total + swap(total, 1 << bit)
        return total[:cut], total[cut:]

    sums, up_bias_grad = sum_all(
        jnp.concatenate(
            [
                output_bias_grad,
                down_bias_grad,
                first_gain_grad,
                first_shift_grad,
                second_gain_grad,
                second_shift_grad,
            ]
        ),
        up_bias0,
        up_bias1,
    )

    out_g0 = blocks(grad(first_low_grad, m0))
    out_g1 = blocks(grad(first_low_grad, m1))

    dq0, dk0, dv0, t0 = attend_back(first_low_grad, output_weight, q0, k0, v0, w0, flip)
    dq1, dk1, dv1, t1 = attend_back(first_low_grad, out_far, q1, k1, v1, w1, flip)
    tokens = x[: seqs * length]

    def input_grads(dq, dk, dv):
        return jnp.concatenate([grad(x, dq), grad(tokens, dk), grad(tokens, dv)], axis=1)

    late0 = jnp.concatenate([out_g0, blocks(input_grads(dq0, dk0, dv0))], axis=2)
    late1 = jnp.concatenate([out_g1, blocks(input_grads(dq1, dk1, dv1))], axis=2)
    late = join(halve(late0, 0, group), halve(late1, 0, group))
    for bit in range(1, bits):
        late = halve(late, bit, group)
    late = late[0].astype(F32)

    def late_small(dq, dk, dv, t):
        spread = jnp.roll(t.reshape(heads, 2 * length), 1, axis=1)
        table = jnp.einsum("bn,hn->bh", onehot, spread, precision=PRECISE)
        return jnp.concatenate(
            [
                jnp.sum(dq.astype(F32), axis=0),
                jnp.sum(dv.astype(F32), axis=0),
                table.reshape(-1),
            ]
        )

    _, small = sum_all(
        jnp.zeros((0,), F32), late_small(dq0, dk0, dv0, t0), late_small(dq1, dk1, dv1, t1)
    )

    x_grad = dot_t(dq0, query_weight) + dot_t(dq1, qkv_far[0])
    token_part = dot_t(dk0, key_weight) + dot_t(dk1, qkv_far[1])
    token_part = token_part + dot_t(dv0, value_weight) + dot_t(dv1, qkv_far[2])
    cut = seqs * length
    low = jnp.concatenate(
        [first_grad[:cut] + x_grad[:cut] + token_part, first_grad[cut:] + x_grad[cut:]], axis=0
    ).astype(BF)
    low_far = across(low)

    def both(mine, theirs):
        lower = jnp.where(side == 0, mine, theirs)
        upper = jnp.where(side == 0, theirs, mine)
        return (
            jnp.concatenate([lower[:cut], upper[:cut]], axis=0),
            jnp.concatenate([lower[cut:], upper[cut:]], axis=0),
        )

    out_c, out_q = both(final_low, final_far)
    grad_c, grad_q = both(low, low_far)
    share = width // group_count
    own = [pick(sums, i * group_count + group, share) for i in range(6)]
    return (
        out_c,
        out_q,
        grad_c.astype(F32),
        grad_q.astype(F32),
        late[:, inner : 2 * inner],
        late[:, 2 * inner : 3 * inner],
        late[:, 3 * inner :],
        late[:, :inner].T,
        up_g[0].astype(F32),
        down_final.T,
        small[:inner],
        small[inner : 2 * inner],
        up_bias_grad,
        small[2 * inner :].reshape(slots, heads),
        own[0],
        own[1],
        own[2],
        own[3],
        own[4],
        own[5],
    )


def solution(mesh):
    in_specs = (
        P("dp", None),
        P("dp", None),
        P("dp", None),
        P(None, "tensor"),
        P(None, "tensor"),
        P(None, "tensor"),
        P("tensor", None),
        P(None, "tensor"),
        P("tensor", None),
        P("tensor"),
        P("tensor"),
        P("tensor"),
        P(),
        P(),
        P(),
        P(),
        P(),
        P(),
        P(None, "tensor"),
        P("dp", None),
        P("dp", None),
    )
    out_specs = (
        P("dp", None),
        P("dp", None),
        P("dp", None),
        P("dp", None),
        P("dp", "tensor"),
        P("dp", "tensor"),
        P("dp", "tensor"),
        P("tensor", "dp"),
        P("dp", "tensor"),
        P("tensor", "dp"),
        P("tensor"),
        P("tensor"),
        P("tensor"),
        P(None, "tensor"),
        P("dp"),
        P("dp"),
        P("dp"),
        P("dp"),
        P("dp"),
        P("dp"),
    )
    return jax.shard_map(body, mesh=mesh, in_specs=in_specs, out_specs=out_specs, check_vma=False)
```

```python
import functools

import jax
import jax.numpy as jnp
from jax import lax
from jax.experimental import pallas as pl
from jax.experimental.pallas import tpu as pltpu
from jax.sharding import PartitionSpec as P

F32 = jnp.float32
BF = jnp.bfloat16
PRECISE = lax.Precision.HIGHEST
EPSILON = 1e-05
THRESHOLDS = (12, 16, 23, 32, 46, 64, 91)


def mm(a,b,ca,cb):
    return lax.dot_general(a,b,(((ca,),(cb,)),((),())),preferred_element_type=F32)

def attend_kernel(picked, x_ref, wq_ref, wk_ref, wv_ref, qb_ref, vb_ref, rank_ref, limit_ref, off_ref,
                  q_ref, k_ref, v_ref, w_ref, m_ref, bias_ref):
    rows=x_ref.shape[0]; length=rank_ref.shape[1]; predict=rows-length; hd=q_ref.shape[1]//2
    x=x_ref[...]
    q=(mm(x,wq_ref[...],1,0)+qb_ref[...]).astype(BF)
    k=mm(x[:length],wk_ref[...],1,0).astype(BF)
    v=(mm(x[:length],wv_ref[...],1,0)+vb_ref[...]).astype(BF)
    q_ref[...]=q; k_ref[...]=k; v_ref[...]=v
    first=lax.broadcasted_iota(jnp.int32,(1,2*hd),1)<hd
    visible=rank_ref[...]<=limit_ref[...]
    parts=[]
    for a in range(2):
        wide=jnp.broadcast_to(off_ref[0,a:a+1,:],(length,2*length))
        turned=pltpu.roll(wide,0,1,stride=1,stride_axis=0)
        bias_ref[:length,:]=turned[:,length:]
        def row(p,c):
            bias_ref[pl.ds(length+p,1),:]=bias_ref[pl.ds(picked[p],1),:]
            return c
        lax.fori_loop(0,predict,row,0,unroll=8)
        mask=first if a==0 else jnp.logical_not(first)
        qa=jnp.where(mask,q,jnp.zeros_like(q))
        s=mm(qa,k,1,1)*0.125+bias_ref[...]
        s=jnp.where(visible,s,-1e30)
        e=jnp.exp(s-jnp.max(s,axis=1,keepdims=True))
        w=(e/jnp.sum(e,axis=1,keepdims=True)).astype(BF)
        w_ref[a]=w
        parts.append(mm(w,v,1,0))
    m_ref[...]=jnp.where(first,parts[0],parts[1]).astype(BF)

def attend(x,wq,wk,wv,qb,vb,rank,limit,off,picked):
    rows,d=x.shape; length=rank.shape[1]; inner=wq.shape[1]; pairs=off.shape[0]; pw=inner//pairs
    col=lambda n:pl.BlockSpec((n,pw),lambda h,p:(0,h))
    full=lambda a:pl.BlockSpec(a.shape,lambda h,p:(0,)*a.ndim)
    s=jax.ShapeDtypeStruct
    return pl.pallas_call(attend_kernel,
        out_shape=(s((rows,inner),BF),s((length,inner),BF),s((length,inner),BF),s((2*pairs,rows,length),BF),s((rows,inner),BF)),
        grid_spec=pltpu.PrefetchScalarGridSpec(num_scalar_prefetch=1,grid=(pairs,),
            in_specs=[full(x),col(d),col(d),col(d),col(1),col(1),full(rank),full(limit),pl.BlockSpec((1,)+off.shape[1:],lambda h,p:(h,0,0))],
            out_specs=(col(rows),col(length),col(length),pl.BlockSpec((2,rows,length),lambda h,p:(h,0,0)),col(rows)),
            scratch_shapes=[pltpu.VMEM((rows,length),F32)]),
        compiler_params=pltpu.CompilerParams(vmem_limit_bytes=56<<20),
        cost_estimate=pl.CostEstimate(flops=2*rows*d*inner*3+4*rows*length*inner,bytes_accessed=20<<20,transcendentals=rows*length*2*pairs),
        name="attend")(picked,x,wq,wk,wv,qb,vb,rank,limit,off)

def back_kernel(g_ref, wo_ref, q_ref, k_ref, v_ref, w_ref, flip_ref, dq_ref, dk_ref, dv_ref, t_ref):
    rows=g_ref.shape[0]; length=k_ref.shape[0]; predict=rows-length; hd=q_ref.shape[1]//2
    do=mm(g_ref[...],wo_ref[...],1,1).astype(BF)
    q=q_ref[...]; k=k_ref[...]; v=v_ref[...]
    first=lax.broadcasted_iota(jnp.int32,(1,2*hd),1)<hd
    dq=[];dk=[];dv=[]
    for a in range(2):
        mask=first if a==0 else jnp.logical_not(first)
        doa=jnp.where(mask,do,jnp.zeros_like(do))
        wl=w_ref[a]; w=wl.astype(F32)
        dw=mm(doa,v,1,1)
        centre=jnp.sum(dw*w,axis=1,keepdims=True)
        ds=(w*(dw-centre)).astype(BF)
        dq.append(mm(ds,k,1,0)); dk.append(mm(ds,q,0,0)); dv.append(mm(wl,do,0,0))
        flipped=mm(flip_ref[...],ds,1,0)
        wide=jnp.concatenate([flipped,jnp.zeros((length,length),F32)],axis=1)
        turned=pltpu.roll(wide,0,1,stride=1,stride_axis=0)
        t_ref[0,a:a+1,:]=jnp.sum(turned,axis=0,keepdims=True)
    dq_ref[...]=(jnp.where(first,dq[0],dq[1])*0.125).astype(BF)
    dk_ref[...]=(jnp.where(first,dk[0],dk[1])*0.125).astype(BF)
    dv_ref[...]=jnp.where(first,dv[0],dv[1]).astype(BF)

def attend_back(g,wo,q,k,v,w,flip):
    rows,d=g.shape; length,inner=k.shape; pairs=w.shape[0]//2; pw=inner//pairs
    col=lambda n:pl.BlockSpec((n,pw),lambda h:(0,h))
    s=jax.ShapeDtypeStruct
    return pl.pallas_call(back_kernel,
        out_shape=(s((rows,inner),BF),s((length,inner),BF),s((length,inner),BF),s((pairs,2,2*length),F32)),
        grid=(pairs,),
        in_specs=[pl.BlockSpec((rows,d),lambda h:(0,0)),pl.BlockSpec((pw,d),lambda h:(h,0)),col(rows),col(length),col(length),pl.BlockSpec((2,rows,length),lambda h:(h,0,0)),pl.BlockSpec(flip.shape,lambda h:(0,0))],
        out_specs=(col(rows),col(length),col(length),pl.BlockSpec((1,2,2*length),lambda h:(h,0,0))),
        compiler_params=pltpu.CompilerParams(vmem_limit_bytes=56<<20),
        cost_estimate=pl.CostEstimate(flops=2*rows*d*inner+10*rows*length*inner,bytes_accessed=20<<20,transcendentals=0),
        name="attend_back")(g,wo,q,k,v,w,flip)


def norm_forward(residual, gain_vector, shift_vector):
    center = residual - jnp.mean(residual, axis=-1, keepdims=True)
    spread = jnp.mean(center * center, axis=-1, keepdims=True)
    inverse = lax.rsqrt(spread + EPSILON)
    normed = center * inverse
    return (normed * gain_vector + shift_vector, normed, inverse)


def norm_backward(upstream, normed, inverse, gain_vector):
    scaled = upstream * gain_vector
    inner_term = (
        scaled
        - jnp.mean(scaled, axis=-1, keepdims=True)
        - normed * jnp.mean(scaled * normed, axis=-1, keepdims=True)
    )
    return (inner_term * inverse, jnp.sum(upstream * normed, axis=0), jnp.sum(upstream, axis=0))


def gelu_exact(operand):
    return jax.nn.gelu(operand, approximate=False)


def offset_onehot(slots, length):
    offset = jnp.arange(2 * length, dtype=jnp.int32) - length
    distance = jnp.abs(offset)
    bucket = jnp.minimum(distance, 8)
    for threshold in THRESHOLDS:
        bucket = bucket + (distance >= threshold).astype(jnp.int32)
    bucket = bucket + 16 * (offset > 0).astype(jnp.int32)
    return (bucket[None, :] == jnp.arange(slots, dtype=jnp.int32)[:, None]).astype(F32)


def pick(matrix, index, count):
    return lax.dynamic_slice_in_dim(matrix, index * count, count, 0)


def across(value):
    return lax.ppermute(value, "tensor", [(0, 1), (1, 0)])


def swap(value, bit):
    return lax.ppermute(value, "dp", [(i, i ^ bit) for i in range(lax.axis_size("dp"))])


def fetch_half(shard, core):
    halves = shard.reshape((2, shard.shape[0] // 2) + shard.shape[1:])
    return across(lax.dynamic_index_in_dim(halves, core, 0, keepdims=False))


def trade(got, core):
    traded = swap(got, 1)
    low = jnp.where(core == 0, got, traded)
    high = jnp.where(core == 0, traded, got)
    return jnp.concatenate([low, high], axis=0)


def reduce_kernel(orders, parts, small_rows, *refs):
    count = len(parts)
    hbm = refs[:count]
    own_ref, oth_ref = refs[count : count + 2]
    outs = refs[count + 2 : 2 * count + 2]
    small_out = refs[2 * count + 2]
    rest = refs[2 * count + 3 :]
    stages = len(orders[0])
    now = [rest[j * stages : (j + 1) * stages] for j in range(count)]
    rest = rest[count * stages :]
    got = [rest[j * stages : (j + 1) * stages] for j in range(count)]
    rest = rest[count * stages :]
    vec_now, vec_got, send_sem, recv_sem, load_sem, vec_send, vec_recv = rest
    group = lax.axis_index("dp")
    side = lax.axis_index("tensor")
    far = stages - 1

    def mine(bit):
        return 0 if bit == far else (group // (1 << bit)) % 2

    def partner(bit):
        if bit == far:
            return (group, 1 - side)
        return (group + (1 << bit) - (2 << bit) * mine(bit), side)

    barrier = pltpu.get_barrier_semaphore()
    for bit in range(stages):
        pl.semaphore_signal(
            barrier, inc=1, device_id=partner(bit), device_id_type=pl.DeviceIdType.MESH
        )
    pl.semaphore_wait(barrier, stages)

    def place(j, stage):
        order = orders[j]
        return sum(1 for later in order[stage + 1 :] if later < order[stage])

    def at(i, spot, value):
        low = 1 << spot
        return (i // low) * (2 * low) + value * low + i % low

    def send(j, stage):
        bit = orders[j][stage]
        spot = place(j, stage)
        source = hbm[j] if stage == 0 else now[j][stage - 1]
        target = got[j][stage]

        def one(i, carry):
            pltpu.make_async_remote_copy(
                src_ref=source.at[at(i, spot, 1 - mine(bit))],
                dst_ref=target.at[i],
                send_sem=send_sem.at[j, stage],
                recv_sem=recv_sem.at[j, stage],
                device_id=partner(bit),
                device_id_type=pl.DeviceIdType.MESH,
            ).start()
            return carry

        lax.fori_loop(0, target.shape[0], one, 0)

    def whole(j, stage):
        target = got[j][stage]
        return pltpu.make_async_remote_copy(
            src_ref=target,
            dst_ref=target,
            send_sem=send_sem.at[j, stage],
            recv_sem=recv_sem.at[j, stage],
            device_id=partner(orders[j][stage]),
            device_id_type=pl.DeviceIdType.MESH,
        )

    def vec_copy(stage):
        return pltpu.make_async_remote_copy(
            src_ref=oth_ref if stage == 0 else vec_now.at[stage - 1],
            dst_ref=vec_got.at[stage],
            send_sem=vec_send.at[stage],
            recv_sem=vec_recv.at[stage],
            device_id=partner(far if stage == 0 else stage - 1),
            device_id_type=pl.DeviceIdType.MESH,
        )

    for j in range(count):
        send(j, 0)
    vec_copy(0).start()
    for j in range(count):

        def load(i, carry):
            pltpu.make_async_copy(
                hbm[j].at[at(i, place(j, 0), mine(orders[j][0]))], now[j][0].at[i], load_sem.at[j]
            ).start()
            return carry

        lax.fori_loop(0, now[j][0].shape[0], load, 0)
    for stage in range(stages):
        for j in range(count):
            if stage == 0:
                pltpu.make_async_copy(got[j][0], now[j][0], load_sem.at[j]).wait()
            whole(j, stage).wait_recv()
            bit = orders[j][stage]
            spot = place(j, stage)
            last = stage == stages - 1
            source = now[j][0] if stage == 0 else now[j][stage - 1]

            def add(i, carry):
                index = i if stage == 0 else at(i, spot, mine(bit))
                total = source[index].astype(F32) + got[j][stage][i].astype(F32)
                if last:
                    outs[j][...] = total
                else:
                    now[j][stage][i] = total.astype(BF)
                return carry

            lax.fori_loop(0, got[j][stage].shape[0], add, 0)
            if not last:
                send(j, stage + 1)
        vec_copy(stage).wait_recv()
        before = own_ref[...] if stage == 0 else vec_now[stage - 1]
        total = before + vec_got[stage]
        if stage == stages - 1:
            small_out[...] = total
        else:
            vec_now[stage] = total
            vec_copy(stage + 1).start()
    for stage in range(stages):
        for j in range(count):
            whole(j, stage).wait_send()
        vec_copy(stage).wait_send()


def reduce_all(parts, own, oth, orders):
    stages = len(orders[0])
    now, got = [], []
    for part in parts:
        total, rows, columns = part.shape
        sizes = [total >> (stage + 1) for stage in range(stages)]
        now += [pltpu.VMEM((size, rows, columns), BF) for size in sizes]
        got += [pltpu.VMEM((size, rows, columns), BF) for size in sizes]
    count = len(parts)
    shape = own.shape
    vmem = pl.BlockSpec(memory_space=pltpu.VMEM)
    dma = pltpu.SemaphoreType.DMA
    return pl.pallas_call(
        functools.partial(reduce_kernel, orders, tuple(p.shape for p in parts), shape[0]),
        out_shape=tuple(jax.ShapeDtypeStruct(p.shape[1:], F32) for p in parts)
        + (jax.ShapeDtypeStruct(shape, F32),),
        in_specs=[pl.BlockSpec(memory_space=pltpu.HBM)] * count + [vmem, vmem],
        out_specs=(vmem,) * (count + 1),
        scratch_shapes=now
        + got
        + [
            pltpu.VMEM((stages,) + shape, F32),
            pltpu.VMEM((stages,) + shape, F32),
            dma((count, stages)),
            dma((count, stages)),
            dma((count,)),
            dma((stages,)),
            dma((stages,)),
        ],
        compiler_params=pltpu.CompilerParams(
            collective_id=0, has_side_effects=True, vmem_limit_bytes=60 << 20
        ),
        name="reduce_all",
    )(*parts, own, oth)


def body(
    content,
    query_stream,
    factor_order,
    query_weight,
    key_weight,
    value_weight,
    output_weight,
    up_weight,
    down_weight,
    query_bias,
    value_bias,
    up_bias,
    output_bias,
    down_bias,
    first_gain,
    first_shift,
    second_gain,
    second_shift,
    bucket_table,
    content_cotangent,
    query_cotangent,
):
    side = lax.axis_index("tensor")
    group = lax.axis_index("dp")
    group_count = lax.axis_size("dp")
    bits = group_count.bit_length() - 1
    core = group & 1
    length = factor_order.shape[1]
    predict = query_stream.shape[0] // factor_order.shape[0]
    seqs = factor_order.shape[0] // 2
    x = jnp.concatenate(
        [pick(content, side, seqs * length), pick(query_stream, side, seqs * predict)], axis=0
    )
    upstream = jnp.concatenate(
        [pick(content_cotangent, side, seqs * length), pick(query_cotangent, side, seqs * predict)],
        axis=0,
    )
    order = pick(factor_order, side, seqs)[0]
    width = x.shape[1]
    inner = query_weight.shape[1]
    heads = bucket_table.shape[1]
    slots = bucket_table.shape[0]

    packed = jnp.concatenate([query_bias, value_bias, up_bias, bucket_table.T.reshape(-1)])
    far = across(packed)

    def unpack(vector):
        a, b, c = inner, 2 * inner, 2 * inner + up_bias.shape[0]
        return vector[:a], vector[a:b], vector[b:c], vector[c:].reshape(heads, slots)

    qkv = jnp.stack([query_weight, key_weight, value_weight])
    qkv_far = trade(fetch_half(qkv.reshape(3 * width, inner), core), core).reshape(3, width, inner)
    out_far = trade(fetch_half(output_weight, core), core)
    up_got = fetch_half(up_weight, core)
    down_got = fetch_half(down_weight, core)

    onehot = offset_onehot(slots, length)
    positions = jnp.arange(length, dtype=jnp.int32)
    rank = jnp.sum(
        jnp.where(order[:, None] == positions[None, :], positions[:, None], 0), axis=0
    ).astype(jnp.int32)
    picked = order[length - predict :]
    limit = jnp.concatenate(
        [
            jnp.maximum(rank, length - predict - 1),
            length - predict - 1 + jnp.arange(predict, dtype=jnp.int32),
        ]
    )[:, None]
    rank = rank[None, :]
    source = jnp.concatenate([positions, picked])
    flip = (source[None, :] == length - 1 - positions[:, None]).astype(BF)

    def attend_half(weights, small):
        qb, vb, _, table = small
        offsets = jnp.einsum("hb,bn->hn", table, onehot, precision=PRECISE)
        return attend(
            x,
            weights[0],
            weights[1],
            weights[2],
            qb[None, :],
            vb[None, :],
            rank,
            limit,
            offsets.reshape(heads // 2, 2, 2 * length),
            picked,
        )

    near_small = unpack(packed)
    far_small = unpack(far)
    q0, k0, v0, w0, m0 = attend_half((query_weight, key_weight, value_weight), near_small)
    q1, k1, v1, w1, m1 = attend_half((qkv_far[0], qkv_far[1], qkv_far[2]), far_small)

    m1, up_got, down_got = lax.optimization_barrier((m1, up_got, down_got))
    up_far = trade(up_got, core)
    down_far = trade(down_got, core)

    def dot(a, b):
        return jnp.dot(a, b, preferred_element_type=F32)

    def dot_t(a, b):
        return lax.dot_general(a, b, (((1,), (1,)), ((), ())), preferred_element_type=F32)

    def grad(a, b):
        return lax.dot_general(a, b, (((0,), (0,)), ((), ())), preferred_element_type=F32)

    branch = dot(m0, output_weight) + dot(m1, out_far)
    first_out, first_normed, first_inverse = norm_forward(
        x.astype(F32) + branch + output_bias, first_gain, first_shift
    )
    first_low = first_out.astype(BF)

    def hidden_of(weight, bias):
        pre = dot(first_low, weight) + bias
        value, pull = jax.vjp(gelu_exact, pre)
        return value.astype(BF), pull

    h0, pull0 = hidden_of(up_weight, near_small[2])
    h1, pull1 = hidden_of(up_far, far_small[2])
    feed = dot(h0, down_weight) + dot(h1, down_far)
    final_out, second_normed, second_inverse = norm_forward(
        first_out + feed + down_bias, second_gain, second_shift
    )
    final_low = final_out.astype(BF)
    final_far = across(final_low)
    second_grad, second_gain_grad, second_shift_grad = norm_backward(
        upstream.astype(F32), second_normed, second_inverse, second_gain
    )
    second_low = second_grad.astype(BF)
    down_bias_grad = jnp.sum(second_grad, axis=0)

    def blocks(matrix):
        rows, columns = matrix.shape
        return matrix.astype(BF).reshape(group_count, rows // group_count, columns)

    down_g = jnp.concatenate([blocks(grad(second_low, h0)), blocks(grad(second_low, h1))], axis=0)

    (pre0,) = pull0(dot_t(second_low, down_weight))
    (pre1,) = pull1(dot_t(second_low, down_far))
    p0 = pre0.astype(BF)
    p1 = pre1.astype(BF)
    up_g = jnp.concatenate([blocks(grad(first_low, p0)), blocks(grad(first_low, p1))], axis=0)
    up_bias0 = jnp.sum(p0.astype(F32), axis=0)
    up_bias1 = jnp.sum(p1.astype(F32), axis=0)
    back = dot_t(p0, up_weight) + dot_t(p1, up_far)
    first_grad, first_gain_grad, first_shift_grad = norm_backward(
        second_grad + back, first_normed, first_inverse, first_gain
    )
    first_low_grad = first_grad.astype(BF)
    output_bias_grad = jnp.sum(first_grad, axis=0)

    out_g0 = blocks(grad(first_low_grad, m0))
    out_g1 = blocks(grad(first_low_grad, m1))

    dq0, dk0, dv0, t0 = attend_back(first_low_grad, output_weight, q0, k0, v0, w0, flip)
    dq1, dk1, dv1, t1 = attend_back(first_low_grad, out_far, q1, k1, v1, w1, flip)
    tokens = x[: seqs * length]

    def input_grads(dq, dk, dv):
        return jnp.concatenate([grad(x, dq), grad(tokens, dk), grad(tokens, dv)], axis=1)

    late0 = jnp.concatenate([out_g0, blocks(input_grads(dq0, dk0, dv0))], axis=2)
    late1 = jnp.concatenate([out_g1, blocks(input_grads(dq1, dk1, dv1))], axis=2)
    late_g = jnp.concatenate([late0, late1], axis=0)

    def late_small(dq, dk, dv, t):
        spread = jnp.roll(t.reshape(heads, 2 * length), 1, axis=1)
        table = jnp.einsum("bn,hn->bh", onehot, spread, precision=PRECISE)
        return jnp.concatenate(
            [
                jnp.sum(dq.astype(F32), axis=0),
                jnp.sum(dv.astype(F32), axis=0),
                table.reshape(-1),
            ]
        )

    same = jnp.concatenate(
        [
            output_bias_grad,
            down_bias_grad,
            first_gain_grad,
            first_shift_grad,
            second_gain_grad,
            second_shift_grad,
        ]
    )

    def lanes(*vectors):
        vector = jnp.concatenate(vectors)
        return jnp.pad(vector, (0, -vector.shape[0] % 1024)).reshape(-1, 128)

    own_sums = lanes(same, up_bias0, late_small(dq0, dk0, dv0, t0))
    oth_sums = lanes(same, up_bias1, late_small(dq1, dk1, dv1, t1))
    first = (0, bits) + tuple(range(1, bits))
    second = (0,) + tuple(range(1, 2)) + (bits,) + tuple(range(2, bits))
    third = (0,) + tuple(range(2, bits)) + (bits, 1)
    late, up_sum, down_sum, totals = reduce_all(
        (late_g, up_g, down_g), own_sums, oth_sums, (first, second, third)
    )
    totals = totals.reshape(-1)
    sums = totals[: same.shape[0]]
    cut_b = same.shape[0] + up_bias0.shape[0]
    up_bias_grad = totals[same.shape[0] : cut_b]
    small = totals[cut_b : cut_b + 2 * inner + slots * heads]

    x_grad = dot_t(dq0, query_weight) + dot_t(dq1, qkv_far[0])
    token_part = dot_t(dk0, key_weight) + dot_t(dk1, qkv_far[1])
    token_part = token_part + dot_t(dv0, value_weight) + dot_t(dv1, qkv_far[2])
    cut = seqs * length
    low = jnp.concatenate(
        [first_grad[:cut] + x_grad[:cut] + token_part, first_grad[cut:] + x_grad[cut:]], axis=0
    ).astype(BF)
    low_far = across(low)

    def both(mine, theirs):
        lower = jnp.where(side == 0, mine, theirs)
        upper = jnp.where(side == 0, theirs, mine)
        return (
            jnp.concatenate([lower[:cut], upper[:cut]], axis=0),
            jnp.concatenate([lower[cut:], upper[cut:]], axis=0),
        )

    out_c, out_q = both(final_low, final_far)
    grad_c, grad_q = both(low, low_far)
    share = width // group_count
    own = [pick(sums, i * group_count + group, share) for i in range(6)]
    return (
        out_c,
        out_q,
        grad_c.astype(F32),
        grad_q.astype(F32),
        late[:, inner : 2 * inner],
        late[:, 2 * inner : 3 * inner],
        late[:, 3 * inner :],
        late[:, :inner].T,
        up_sum,
        down_sum.T,
        small[:inner],
        small[inner : 2 * inner],
        up_bias_grad,
        small[2 * inner :].reshape(slots, heads),
        own[0],
        own[1],
        own[2],
        own[3],
        own[4],
        own[5],
    )


def solution(mesh):
    in_specs = (
        P("dp", None),
        P("dp", None),
        P("dp", None),
        P(None, "tensor"),
        P(None, "tensor"),
        P(None, "tensor"),
        P("tensor", None),
        P(None, "tensor"),
        P("tensor", None),
        P("tensor"),
        P("tensor"),
        P("tensor"),
        P(),
        P(),
        P(),
        P(),
        P(),
        P(),
        P(None, "tensor"),
        P("dp", None),
        P("dp", None),
    )
    out_specs = (
        P("dp", None),
        P("dp", None),
        P("dp", None),
        P("dp", None),
        P("dp", "tensor"),
        P("dp", "tensor"),
        P("dp", "tensor"),
        P("tensor", "dp"),
        P("dp", "tensor"),
        P("tensor", "dp"),
        P("tensor"),
        P("tensor"),
        P("tensor"),
        P(None, "tensor"),
        P("dp"),
        P("dp"),
        P("dp"),
        P("dp"),
        P("dp"),
        P("dp"),
    )
    return jax.shard_map(body, mesh=mesh, in_specs=in_specs, out_specs=out_specs, check_vma=False)
```
